256 devices in a mesh: dp: 16 (over y, x_hi, core), tensor: 16 (over x_lo, z).
Axes of the slice: x: 4 (x_hi: 2, x_lo: 2; x = x_hi * 2 + x_lo), y: 4, z: 8, core: 2. Of those that a mesh axis runs over, the one named last changes fastest.
Arguments:
- tokens: bfloat16 [32768, 2304], P(('dp', 'tensor')), may hold values from -6 to 6
- cotangent: bfloat16 [32768, 4096], P('dp', 'tensor'), may hold values from -6 to 6
- pre_gain: float32 [2304], replicated, may hold values from 0.25 to 1.75
- w_query: bfloat16 [2304, 4096], P('dp', 'tensor'), may hold values from -0.375 to 0.375
- key_weight: bfloat16 [2304, 2048], P('dp', 'tensor'), may hold values from -0.375 to 0.375
- value_weight: bfloat16 [2304, 2048], P('dp', 'tensor'), may hold values from -0.125 to 0.125
Outputs:
- attended: bfloat16 [32768, 4096], P('dp', 'tensor')
- grad_tokens: bfloat16 [32768, 2304], P(('dp', 'tensor'))
- grad_query: float32 [2304, 4096], P('dp', 'tensor')
- grad_key: float32 [2304, 2048], P('dp', 'tensor')
- grad_value: float32 [2304, 2048], P('dp', 'tensor')
- grad_pre_gain: float32 [2304], replicated
The draws below stay inside these ranges and needn't reach their ends.
All inputs are finite; a program needn't handle non-finite values.
Results may differ from the reference program's by a relative error of at most 0.019.
The reference program's roundings to bfloat16 on the way count: a program that leaves them out, or rounds other values in their place, can miss the bound.
Values may be sent and summed in bfloat16 or wider, within the bound.
No kernel may reach another device: no remote copies, remote signals or barrier semaphores. Data moves between devices by JAX's collectives and lax.ppermute only.
A program may use at most 192 MiB of HBM per device.

```python
import jax
import jax.numpy as jnp
from jax import lax

MODEL_WIDTH = 2304
QUERY_HEADS = 32
KEY_VALUE_HEADS = 16
HEAD_SIZE = 128
TOK_DEV = 128
SEQ_LEN = 64
TOKENS = 32768
N_DP = 16
N_TENSOR = 16


def block_levels(own_key, dims, cuts, least, high):
    level = 1.0
    for dim, parts in cuts:
        heights = jax.random.uniform(jax.random.fold_in(jax.random.fold_in(own_key, 6), dim), (parts,), jnp.float32, least / len(cuts), high / len(cuts))
        level = level * jnp.repeat(jnp.exp(heights), dims[dim] // parts).reshape((-1,) + (1,) * (len(dims) - 1 - dim))
    return level


def bell_draw(rng, shape, spread, reach, cuts=(), kind=jnp.bfloat16):
    factor_of = block_levels(rng, shape, cuts, -0.22, 0.18) if cuts else 1.0
    result = jax.random.normal(rng, shape, jnp.float32) * spread * factor_of
    return jnp.minimum(jnp.maximum(result, -reach), reach).astype(kind)


def setup_inputs(seed: int = 0) -> dict:
    key_list = jax.random.split(jax.random.key(seed), 7)
    tokens = bell_draw(key_list[0], (TOKENS, MODEL_WIDTH), 1.0, 6.0, ((0, 256),))
    cotangent = bell_draw(key_list[1], (TOKENS, QUERY_HEADS * HEAD_SIZE), 1.0, 6.0, ((0, 16), (1, 16)))
    pre_gain = jnp.clip(1.0 + 0.15 * jax.random.normal(key_list[2], (MODEL_WIDTH,), jnp.float32), 0.25, 1.75)
    w_query = bell_draw(key_list[3], (MODEL_WIDTH, QUERY_HEADS * HEAD_SIZE), (MODEL_WIDTH // 9) ** -0.5, 0.375, ((0, 16), (1, 16)))
    key_weight = bell_draw(key_list[4], (MODEL_WIDTH, KEY_VALUE_HEADS * HEAD_SIZE), (MODEL_WIDTH // 9) ** -0.5, 0.375, ((0, 16), (1, 16)))
    value_weight = bell_draw(key_list[5], (MODEL_WIDTH, KEY_VALUE_HEADS * HEAD_SIZE), MODEL_WIDTH ** -0.5, 0.125, ((0, 16), (1, 16)))
    return {"tokens": tokens, "cotangent": cotangent, "pre_gain": pre_gain, "w_query": w_query, "key_weight": key_weight, "value_weight": value_weight}


EPS = 1e-06
CAP = 50.0
BASE = 10000.0
query_scalar = 144.0

def rotary_tables(segment_length, half):
    places = jnp.arange(segment_length, dtype=jnp.float32)[:, None]
    freqs = BASE ** (-jnp.arange(half, dtype=jnp.float32) / half)
    angles = places * freqs[None, :]
    return (jnp.cos(angles)[:, None, :], jnp.sin(angles)[:, None, :])

def rotate(values, cosine_table, sine_table):
    half = values.shape[-1] // 2
    first, second = (values[..., :half], values[..., half:])
    return jnp.concatenate([first * cosine_table - second * sine_table, second * cosine_table + first * sine_table], -1)

def inverse_rotation(values, cosine_table, sine_table):
    half = values.shape[-1] // 2
    first, second = (values[..., :half], values[..., half:])
    return jnp.concatenate([first * cosine_table + second * sine_table, second * cosine_table - first * sine_table], -1)

def attend_forward(query, key, value):
    repeat = query.shape[1] // key.shape[1]
    keys = jnp.repeat(key, repeat, axis=1).astype(jnp.float32)
    values = jnp.repeat(value, repeat, axis=1).astype(jnp.float32)
    factor = query_scalar ** (-0.5)
    raw = jnp.einsum('qhd,khd->hqk', query.astype(jnp.float32), keys) * factor
    bent = jnp.tanh(raw / CAP)
    capped = CAP * bent
    segment_length = query.shape[0]
    causal = jnp.arange(segment_length)[None, :] <= jnp.arange(segment_length)[:, None]
    raised = jnp.where(causal[None], jnp.exp(capped), 0.0)
    weights = raised / lax.optimization_barrier(jnp.sum(raised, -1, keepdims=True))
    probs = weights.astype(jnp.bfloat16)
    attended = jnp.einsum('hqk,khd->qhd', probs.astype(jnp.float32), values).astype(jnp.bfloat16)
    return (attended, weights, probs, bent)

def attend_backward(d_attended, query, key, value, weights, probs, bent):
    repeat = query.shape[1] // key.shape[1]
    keys = jnp.repeat(key, repeat, axis=1).astype(jnp.float32)
    values = jnp.repeat(value, repeat, axis=1).astype(jnp.float32)
    factor = query_scalar ** (-0.5)
    grad_in = d_attended.astype(jnp.float32)
    d_probs = jnp.einsum('qhd,khd->hqk', grad_in, values)
    d_capped = weights * (d_probs - lax.optimization_barrier(jnp.sum(weights * d_probs, -1, keepdims=True)))
    d_scores = (d_capped * (1.0 - bent * bent) * factor).astype(jnp.bfloat16).astype(jnp.float32)
    query_back = jnp.einsum('hqk,khd->qhd', d_scores, keys)
    key_heads = jnp.einsum('hqk,qhd->khd', d_scores, query.astype(jnp.float32))
    value_heads = jnp.einsum('hqk,qhd->khd', probs.astype(jnp.float32), grad_in)
    segment_length, heads, width = query.shape
    key_rotated_back = key_heads.reshape(segment_length, heads // repeat, repeat, width).sum(2)
    value_returned = value_heads.reshape(segment_length, heads // repeat, repeat, width).sum(2)
    return (query_back, key_rotated_back, value_returned)

def reference(tokens, cotangent, pre_gain, w_query, key_weight, value_weight):
    segment_length = TOK_DEV * N_TENSOR
    token_span = SEQ_LEN
    pieces_count = segment_length // token_span
    query_groups = N_TENSOR
    col_query = QUERY_HEADS * HEAD_SIZE // query_groups
    column_key = KEY_VALUE_HEADS * HEAD_SIZE // query_groups
    cosine_table, sine_table = rotary_tables(token_span, HEAD_SIZE // 2)

    def one_block(carry, pieces):
        rows, cot_rows = pieces
        rows_f = rows.astype(jnp.float32)
        inv_one = lax.rsqrt(lax.optimization_barrier(jnp.mean(rows_f * rows_f, -1, keepdims=True)) + EPS)
        unit_one = rows_f * inv_one
        normed_input = (unit_one * pre_gain).astype(jnp.bfloat16)
        query_raw = jnp.dot(normed_input, w_query, preferred_element_type=jnp.float32).reshape(pieces_count, token_span, QUERY_HEADS, HEAD_SIZE)
        key_unrotated = jnp.dot(normed_input, key_weight, preferred_element_type=jnp.float32).reshape(pieces_count, token_span, KEY_VALUE_HEADS, HEAD_SIZE)
        value_projected = jnp.dot(normed_input, value_weight, preferred_element_type=jnp.float32).reshape(pieces_count, token_span, KEY_VALUE_HEADS, HEAD_SIZE)
        query = rotate(query_raw, cosine_table, sine_table).astype(jnp.bfloat16)
        key = rotate(key_unrotated, cosine_table, sine_table).astype(jnp.bfloat16)
        value = value_projected.astype(jnp.bfloat16)
        attended, weights, probs, bent = jax.vmap(attend_forward)(query, key, value)
        attended = attended.reshape(segment_length, QUERY_HEADS * HEAD_SIZE)
        d_attended = cot_rows.reshape(pieces_count, token_span, QUERY_HEADS, HEAD_SIZE)
        query_back, key_rotated_back, value_returned = jax.vmap(attend_backward)(d_attended, query, key, value, weights, probs, bent)
        d_query = inverse_rotation(query_back, cosine_table, sine_table).astype(jnp.bfloat16).reshape(segment_length, QUERY_HEADS * HEAD_SIZE)
        key_gradient = inverse_rotation(key_rotated_back, cosine_table, sine_table).astype(jnp.bfloat16).reshape(segment_length, KEY_VALUE_HEADS * HEAD_SIZE)
        value_gradient = value_returned.astype(jnp.bfloat16).reshape(segment_length, KEY_VALUE_HEADS * HEAD_SIZE)
        query_part = jnp.dot(normed_input.T, d_query, preferred_element_type=jnp.float32)
        key_part = jnp.dot(normed_input.T, key_gradient, preferred_element_type=jnp.float32)
        value_part = jnp.dot(normed_input.T, value_gradient, preferred_element_type=jnp.float32)
        back = jnp.einsum('lgc,dgc->lgd', d_query.reshape(segment_length, query_groups, col_query).astype(jnp.float32), w_query.reshape(MODEL_WIDTH, query_groups, col_query).astype(jnp.float32))
        back = back + jnp.einsum('lgc,dgc->lgd', key_gradient.reshape(segment_length, query_groups, column_key).astype(jnp.float32), key_weight.reshape(MODEL_WIDTH, query_groups, column_key).astype(jnp.float32))
        back = back + jnp.einsum('lgc,dgc->lgd', value_gradient.reshape(segment_length, query_groups, column_key).astype(jnp.float32), value_weight.reshape(MODEL_WIDTH, query_groups, column_key).astype(jnp.float32))
        back = lax.optimization_barrier(back.astype(jnp.bfloat16))
        d_normed = lax.optimization_barrier(jnp.sum(back.astype(jnp.float32), 1))
        pre_part = lax.optimization_barrier(jnp.sum(d_normed * unit_one, 0))
        scaled_in = d_normed * pre_gain
        grad_rows = (inv_one * (scaled_in - unit_one * lax.optimization_barrier(jnp.mean(scaled_in * unit_one, -1, keepdims=True)))).astype(jnp.bfloat16)
        rounded = lax.optimization_barrier(tuple((part.astype(jnp.bfloat16) for part in (query_part, key_part, value_part))))
        sums = tuple((total + part.astype(jnp.float32) for total, part in zip(carry[:3], rounded)))
        carry = sums + (carry[3] + pre_part,)
        return (carry, (attended, grad_rows))
    start_offset = (jnp.zeros((MODEL_WIDTH, QUERY_HEADS * HEAD_SIZE), jnp.float32), jnp.zeros((MODEL_WIDTH, KEY_VALUE_HEADS * HEAD_SIZE), jnp.float32), jnp.zeros((MODEL_WIDTH, KEY_VALUE_HEADS * HEAD_SIZE), jnp.float32), jnp.zeros((MODEL_WIDTH,), jnp.float32))
    pieces = (tokens.reshape(N_DP, segment_length, MODEL_WIDTH), cotangent.reshape(N_DP, segment_length, QUERY_HEADS * HEAD_SIZE))
    totals, (attended, grad_tokens) = lax.scan(one_block, start_offset, pieces)
    return (attended.reshape(N_DP * segment_length, QUERY_HEADS * HEAD_SIZE), grad_tokens.reshape(N_DP * segment_length, MODEL_WIDTH), totals[0], totals[1], totals[2], totals[3])
```

```python
import jax
import jax.numpy as jnp
from jax import lax
from jax.experimental import pallas as pl
from jax.experimental.pallas import tpu as pltpu
from jax.sharding import Mesh
from jax.sharding import PartitionSpec as P

HEAD = 128
SEQ = 64
EPS = 1e-06
CAP = 50.0
BASE = 10000.0
FACTOR = 144.0**-0.5
CHUNKS = 1
TILE = 256
SUB = 128

Y, XH, CORE, XL, Z = "dp_0", "dp_1", "dp_2", "tensor_0", "tensor_1"
X = (XH, XL)
PAIR = (CORE, XL)
ALL = (Y, XH, CORE, XL, Z)
SWAP = [(0, 1), (1, 0)]


def shift(value, axis, size, step):
    return lax.ppermute(value, axis, [((i + step) % size, i) for i in range(size)])


def trade(value):
    return lax.ppermute(value, PAIR, [(0, 0), (1, 2), (2, 1), (3, 3)])


def trade_other(value):
    return lax.ppermute(value, PAIR, [(2 * c + x, 2 * (1 - x) + c) for c in range(2) for x in range(2)])


def trade_other_back(value):
    return lax.ppermute(value, PAIR, [(2 * (1 - x) + c, 2 * c + x) for c in range(2) for x in range(2)])


def gather_plane(first, second):
    one = jnp.stack([first] + [shift(first, X, 4, s) for s in (1, 2, 3)])
    two = jnp.stack([second] + [shift(second, Y, 4, s) for s in (1, 2, 3)])
    one = jnp.stack([one] + [shift(one, Y, 4, s) for s in (1, 2, 3)])
    two = jnp.stack([two] + [shift(two, X, 4, s) for s in (1, 2, 3)], 1)
    return one, two


def pick(value, place, axis):
    return lax.dynamic_index_in_dim(value, place % value.shape[axis], axis, keepdims=False)


def others(terms, name):
    size = len(terms)
    return [shift(terms[size - s], name, size, s) for s in range(1, size)]


def total(first, rest):
    return sum((r.astype(jnp.float32) for r in rest), first.astype(jnp.float32))


def narrow(terms):
    return [terms[0]] + [t.astype(jnp.bfloat16) for t in terms[1:]]


def assemble_kernel(place_ref, one_ref, two_ref, one_other_ref, two_other_ref, w_ref):
    depth = one_ref.shape[2]
    half = one_ref.shape[3]
    y0, x0, core = place_ref[0], place_ref[1], place_ref[2]
    for dy in range(4):
        for dx in range(4):
            y, x = lax.rem(y0 + dy, 4), lax.rem(x0 + dx, 4)
            for refs, c in (((one_ref, two_ref), core), ((one_other_ref, two_other_ref), 1 - core)):
                row = pl.multiple_of(((y * 2 + x // 2) * 2 + c) * depth, 16)
                for k in range(2):
                    col = pl.multiple_of((lax.rem(x, 2) * 2 + k) * half, 128)
                    w_ref[pl.ds(row, depth), pl.ds(col, half)] = refs[k][dy, dx]


def assemble(place, one, two, one_other, two_other):
    depth, half = one.shape[2:]
    whole = pl.BlockSpec(memory_space=pltpu.VMEM)
    return pl.pallas_call(
        assemble_kernel,
        in_specs=[pl.BlockSpec(memory_space=pltpu.SMEM)] + [whole] * 4,
        out_specs=whole,
        out_shape=jax.ShapeDtypeStruct((16 * depth, 4 * half), jnp.bfloat16),
        cost_estimate=pl.CostEstimate(flops=4_000_000_000, bytes_accessed=4 * one.size * 4, transcendentals=0),
        compiler_params=pltpu.CompilerParams(vmem_limit_bytes=32 * 1024 * 1024),
        name="assemble",
    )(place, one, two, one_other, two_other)


def grads_kernel(place_ref, x_ref, d_ref, own_q_ref, own_r_ref, other_q_ref, other_r_ref, dw_ref):
    depth, half = own_q_ref.shape[2:]
    y0, x0, core = place_ref[0], place_ref[1], place_ref[2]
    part = dw_ref.shape[0]
    for p in range(x_ref.shape[1] // part):
        dw_ref[...] = dot(x_ref[:, p * part : (p + 1) * part], d_ref[...], ((0,), (0,)))
        for b in range(part // depth):
            block_row = p * (part // depth) + b
            y, xh, c = block_row // 4, block_row // 2 % 2, block_row % 2
            for xl in range(2):
                dy = lax.rem(y + 4 - y0, 4)
                dx = lax.rem(2 * xh + xl + 4 - x0, 4)
                rows = slice(b * depth, (b + 1) * depth)
                for k, (own, other) in enumerate(((own_q_ref, other_q_ref), (own_r_ref, other_r_ref))):
                    cols = slice((2 * xl + k) * half, (2 * xl + k + 1) * half)
                    value = dw_ref[rows, cols].astype(jnp.bfloat16)
                    at = (dx, dy) if k == 0 else (dy, dx)

                    @pl.when(core == c)
                    def _():
                        own[at[0], at[1]] = value

                    @pl.when(core != c)
                    def _():
                        other[at[0], at[1]] = value


def projection_grads(place, x, d, depth, half):
    whole = pl.BlockSpec(memory_space=pltpu.VMEM)
    out = jax.ShapeDtypeStruct((4, 4, depth, half), jnp.bfloat16)
    return pl.pallas_call(
        grads_kernel,
        in_specs=[pl.BlockSpec(memory_space=pltpu.SMEM), whole, whole],
        out_specs=[whole] * 4,
        out_shape=[out] * 4,
        scratch_shapes=[pltpu.VMEM((x.shape[1] // 2, d.shape[1]), jnp.float32)],
        cost_estimate=pl.CostEstimate(
            flops=2 * x.shape[0] * x.shape[1] * d.shape[1], bytes_accessed=2 * (x.size + d.size) + 8 * out.size, transcendentals=0
        ),
        compiler_params=pltpu.CompilerParams(vmem_limit_bytes=48 * 1024 * 1024),
        name="grads",
    )(place, x, d)


def cyclic_total(value, rest, name):
    size = len(rest) + 1
    every = jnp.concatenate([value] + rest)
    twice = jnp.concatenate([every, every])
    me = lax.axis_index(name)
    return jnp.sum(lax.dynamic_slice_in_dim(twice, (size - me) % size, size), 0, keepdims=True)


def rotary_tables():
    places = jnp.arange(SEQ, dtype=jnp.float32)[:, None]
    half = HEAD // 2
    freqs = BASE ** (-jnp.arange(half, dtype=jnp.float32) / half)
    angles = places * freqs[None, :]
    cosine, sine = jnp.cos(angles), jnp.sin(angles)
    cosine = jnp.concatenate([cosine, cosine], 1)
    sine = jnp.concatenate([-sine, sine], 1)
    return jnp.tile(cosine, (SUB // SEQ, 1)), jnp.tile(sine, (SUB // SEQ, 1))


def dot(a, b, dims):
    return lax.dot_general(a, b, (dims, ((), ())), preferred_element_type=jnp.float32)


def block_kernel(x_ref, w_ref, cot_ref, cos_ref, sin_ref, att_ref, dqkv_ref, dn_ref, gain_ref, qkv_ref):
    qkv_ref[...] = dot(x_ref[...], w_ref[...], ((1,), (0,)))
    cosine, sine = cos_ref[...], sin_ref[...]
    cosine2 = jnp.concatenate([cosine, cosine], 0)
    sine2 = jnp.concatenate([sine, sine], 0)
    row = lax.broadcasted_iota(jnp.int32, (2 * SUB, SUB), 0) % SUB
    col = lax.broadcasted_iota(jnp.int32, (2 * SUB, SUB), 1)
    seen = (col <= row) & (col // SEQ == row // SEQ)
    for t in range(TILE // SUB):
        rows = slice(t * SUB, (t + 1) * SUB)
        for s in range(2):
            base = s * 4 * HEAD
            q = jnp.concatenate(
                [qkv_ref[rows, base : base + HEAD], qkv_ref[rows, base + HEAD : base + 2 * HEAD]], 0
            )
            k = qkv_ref[rows, base + 2 * HEAD : base + 3 * HEAD]
            v = qkv_ref[rows, base + 3 * HEAD : base + 4 * HEAD].astype(jnp.bfloat16)
            q = (q * cosine2 + pltpu.roll(q, HEAD // 2, 1) * sine2).astype(jnp.bfloat16)
            k = (k * cosine + pltpu.roll(k, HEAD // 2, 1) * sine).astype(jnp.bfloat16)
            cot = cot_ref[s, :, 0].reshape(TILE, 2 * HEAD)[rows]
            cot = jnp.concatenate([cot[:, :HEAD], cot[:, HEAD:]], 0)
            bent = jnp.tanh(dot(q, k, ((1,), (1,))) * (FACTOR / CAP))
            raised = jnp.where(seen, jnp.exp(CAP * bent), 0.0)
            weights = raised / jnp.sum(raised, -1, keepdims=True)
            probs = weights.astype(jnp.bfloat16)
            att = dot(probs, v, ((1,), (0,))).astype(jnp.bfloat16)
            for h in range(2):
                att_ref[s, 2 * t : 2 * t + 2, :, h * HEAD : (h + 1) * HEAD] = att[h * SUB : (h + 1) * SUB].reshape(
                    2, SEQ, HEAD
                )
            d_probs = dot(cot, v, ((1,), (1,)))
            inner = jnp.sum(weights * d_probs, -1, keepdims=True)
            d_scores = (weights * (d_probs - inner) * (1.0 - bent * bent) * FACTOR).astype(jnp.bfloat16)
            dq = dot(d_scores, k, ((1,), (0,)))
            dk = dot(d_scores, q, ((0,), (0,)))
            dv = dot(probs, cot, ((0,), (0,)))
            dq = (dq * cosine2 - pltpu.roll(dq, HEAD // 2, 1) * sine2).astype(jnp.bfloat16)
            dk = (dk * cosine - pltpu.roll(dk, HEAD // 2, 1) * sine).astype(jnp.bfloat16)
            dqkv_ref[rows, base : base + HEAD] = dq[:SUB]
            dqkv_ref[rows, base + HEAD : base + 2 * HEAD] = dq[SUB:]
            dqkv_ref[rows, base + 2 * HEAD : base + 3 * HEAD] = dk
            dqkv_ref[rows, base + 3 * HEAD : base + 4 * HEAD] = dv.astype(jnp.bfloat16)
    dn = dot(dqkv_ref[...], w_ref[...], ((1,), (1,)))
    dn_ref[...] = dn.astype(jnp.bfloat16)
    part = jnp.sum(dn * x_ref[...].astype(jnp.float32), 0, keepdims=True)

    @pl.when(pl.program_id(0) == 0)
    def _():
        gain_ref[...] = part

    @pl.when(pl.program_id(0) > 0)
    def _():
        gain_ref[...] += part


def block(x, w, cot, cosine, sine, chunk):
    rows, width = x.shape
    columns = w.shape[1]
    per = TILE // SEQ
    full = lambda shape: pl.BlockSpec(shape, lambda i: (0,) * len(shape))
    tile = lambda n: pl.BlockSpec((TILE, n), lambda i: (i, 0))
    flops = 4 * rows * width * columns + 12 * rows * SUB * columns
    return pl.pallas_call(
        block_kernel,
        grid=(rows // TILE,),
        in_specs=[
            tile(width),
            full((width, columns)),
            pl.BlockSpec((2, per, 1, SEQ, 2 * HEAD), lambda i: (0, i, chunk, 0, 0)),
            full((SUB, HEAD)),
            full((SUB, HEAD)),
        ],
        out_specs=[
            pl.BlockSpec((2, per, SEQ, 2 * HEAD), lambda i: (0, i, 0, 0)),
            tile(columns),
            tile(width),
            full((1, width)),
        ],
        out_shape=[
            jax.ShapeDtypeStruct((2, rows // SEQ, SEQ, 2 * HEAD), jnp.bfloat16),
            jax.ShapeDtypeStruct((rows, columns), jnp.bfloat16),
            jax.ShapeDtypeStruct((rows, width), jnp.bfloat16),
            jax.ShapeDtypeStruct((1, width), jnp.float32),
        ],
        scratch_shapes=[pltpu.VMEM((TILE, columns), jnp.float32)],
        cost_estimate=pl.CostEstimate(
            flops=flops, bytes_accessed=2 * (2 * rows * width + width * columns + 3 * rows * columns), transcendentals=0
        ),
        compiler_params=pltpu.CompilerParams(vmem_limit_bytes=48 * 1024 * 1024),
        name="block",
    )(x, w, cot, cosine, sine)


def per_device(tokens, cotangent, pre_gain, w_query, key_weight, value_weight):
    c, x = lax.axis_index(CORE), lax.axis_index(XL)
    depth = w_query.shape[0]
    own = tokens.shape[0]
    per_chunk = own // CHUNKS

    normed, units, inverses = [], [], []
    for j in range(CHUNKS):
        rows = trade(tokens[j * per_chunk : (j + 1) * per_chunk]).astype(jnp.float32)
        inv_one = lax.rsqrt(jnp.mean(rows * rows, -1, keepdims=True) + EPS)
        unit_one = rows * inv_one
        normed.append((unit_one * pre_gain).astype(jnp.bfloat16))
        units.append(unit_one)
        inverses.append(inv_one)
    gathered = [lax.all_gather(n, Z, axis=0, tiled=True) for n in normed]

    place = jnp.stack([lax.axis_index(Y), lax.axis_index(X), c])
    one, two = gather_plane(w_query, jnp.concatenate([key_weight, value_weight], 1))
    weight = assemble(place, one, two, lax.ppermute(one, CORE, SWAP), lax.ppermute(two, CORE, SWAP))

    halves = cotangent.reshape(2, -1, cotangent.shape[1])
    same = trade(pick(halves, x, 0))
    cross = trade_other(pick(halves, 1 - x, 0))
    cot = jnp.where(c == 0, jnp.stack([same, cross]), jnp.stack([cross, same]))
    cot = cot.reshape(2, -1, CHUNKS, SEQ, cot.shape[-1])

    cosine, sine = rotary_tables()
    attended, joined, scattered, gain = [], [], [], 0.0
    for j in range(CHUNKS):
        att, dqkv, dn, part = block(gathered[j], weight, cot, cosine, sine, j)
        attended.append(att)
        joined.append(dqkv)
        gain = gain + part
        scattered.append(lax.psum_scatter(dn, Z, scatter_dimension=0, tiled=True))

    gain = cyclic_total(gain, others([gain] * 8, Z), Z)

    att = jnp.stack(attended, 2).reshape(2, -1, 2 * HEAD)
    same = trade(pick(att, c, 0))
    cross = trade_other_back(pick(att, 1 - c, 0))
    attended_flat = jnp.where(x == 0, jnp.concatenate([same, cross]), jnp.concatenate([cross, same]))

    own_q, own_r, other_q, other_r = projection_grads(
        place, jnp.concatenate(gathered), jnp.concatenate(joined), depth, w_query.shape[1]
    )
    barrier = lax.optimization_barrier
    own_q, other_q, gain = barrier((own_q, other_q, gain))
    got_q, got_r, got_gain = barrier(tuple(lax.ppermute(v, CORE, SWAP) for v in (other_q, other_r, gain)))
    gain = gain + got_gain
    both = lambda a, b: [a[r].astype(jnp.float32) + b[r].astype(jnp.float32) for r in range(4)]
    one, two = narrow(both(own_q, got_q)), narrow(both(own_r, got_r))
    got_q, got_r, got_gain = barrier((others(one, X), others(two, Y), others([gain] * 4, X)))
    gain = cyclic_total(gain, got_gain, X)
    one, two = narrow(list(total(one[0], got_q))), narrow(list(total(two[0], got_r)))
    got_q, got_r, got_gain = others(one, Y), others(two, X), others([gain] * 4, Y)
    gain = cyclic_total(gain, got_gain, Y)
    grad_query, grad_rest = total(one[0], got_q), total(two[0], got_r)
    few = key_weight.shape[1]
    grad_key, grad_value = grad_rest[:, :few], grad_rest[:, few:]
    grad_pre = gain[0] / pre_gain

    grad_rows = []
    for j in range(CHUNKS):
        d_normed = scattered[j].astype(jnp.float32)
        scaled = d_normed * pre_gain
        out = inverses[j] * (scaled - units[j] * jnp.mean(scaled * units[j], -1, keepdims=True))
        grad_rows.append(trade(out.astype(jnp.bfloat16)))
    return (attended_flat, jnp.concatenate(grad_rows), grad_query, grad_key, grad_value, grad_pre)


def solution(mesh):
    torus = Mesh(mesh.devices.reshape(4, 2, 2, 2, 8), ALL)
    dp, tensor = (Y, XH, CORE), (XL, Z)
    in_specs = (P(ALL, None), P(dp, tensor), P(), P(dp, tensor), P(dp, tensor), P(dp, tensor))
    out_specs = (P(dp, tensor), P(ALL, None), P(dp, tensor), P(dp, tensor), P(dp, tensor), P())
    return jax.shard_map(per_device, mesh=torus, in_specs=in_specs, out_specs=out_specs, check_vma=False)
```

```python
import functools

import jax
import jax.numpy as jnp
import numpy as np
from jax import lax
from jax.experimental import pallas as pl
from jax.experimental.pallas import tpu as pltpu
from jax.sharding import Mesh
from jax.sharding import PartitionSpec as P

HEAD = 128
SEQ = 64
EPS = 1e-06
CAP = 50.0
BASE = 10000.0
FACTOR = 144.0**-0.5
TILE = 256
SUB = 128

Y, XH, CORE, XL, Z = "dp_0", "dp_1", "dp_2", "tensor_0", "tensor_1"
X = (XH, XL)
ALL = (Y, XH, CORE, XL, Z)
SWAP = [(0, 1), (1, 0)]


def shift(value, axis, size, step):
    return lax.ppermute(value, axis, [((i + step) % size, i) for i in range(size)])


def gather_plane(own):
    row = jnp.stack([own] + [shift(own, X, 4, s) for s in (1, 2, 3)])
    return jnp.stack([row] + [shift(row, Y, 4, s) for s in (1, 2, 3)])


def pick(value, place, axis):
    return lax.dynamic_index_in_dim(value, place % value.shape[axis], axis, keepdims=False)


def others(terms, name):
    size = len(terms)
    return [shift(terms[size - s], name, size, s) for s in range(1, size)]


def total(first, rest):
    return sum((r.astype(jnp.float32) for r in rest), first.astype(jnp.float32))


def narrow(terms):
    return [terms[0]] + [t.astype(jnp.bfloat16) for t in terms[1:]]


def assemble(place_ref, own_ref, other_ref, w_ref):
    depth, wide = own_ref.shape[2:]
    y0, x0, core = place_ref[0], place_ref[1], place_ref[2]

    @pl.loop(0, 16)
    def _(i):
        dy, dx = i // 4, lax.rem(i, 4)
        y, x = lax.rem(y0 + dy, 4), lax.rem(x0 + dx, 4)
        col = pl.multiple_of(lax.rem(x, 2) * wide, 128)
        for ref, c in ((own_ref, core), (other_ref, 1 - core)):
            row = pl.multiple_of(((y * 2 + x // 2) * 2 + c) * depth, 16)
            w_ref[pl.ds(row, depth), pl.ds(col, wide)] = ref[dy, dx]


def grads_kernel(place_ref, x_ref, d_ref, own_ref, other_ref, dw_ref):
    depth, wide = own_ref.shape[3:]
    y0, x0, core = place_ref[0], place_ref[1], place_ref[2]
    step = pl.program_id(0)
    part = x_ref.shape[1]
    steps = dw_ref.shape[0] // part
    at = pl.ds(pl.multiple_of(lax.rem(step, steps) * part, part), part)
    dw_ref[at, :] = dot(x_ref[...], d_ref[...], ((0,), (0,)))

    @pl.when(lax.rem(step, steps) == steps - 1)
    def _():
        blocks = dw_ref.shape[0] // depth

        @pl.loop(0, blocks)
        def _(i):
            b = step // steps * blocks + i
            y, xh, c = b // 4, lax.rem(b // 2, 2), lax.rem(b, 2)
            rows = pl.ds(pl.multiple_of(i * depth, 16), depth)
            for xl in range(2):
                dy = lax.rem(y + 4 - y0, 4)
                dx = lax.rem(2 * xh + xl + 4 - x0, 4)
                for half, at in enumerate(((dx, dy), (dy, dx))):
                    col = (2 * xl + half) * wide
                    value = dw_ref[rows, col : col + wide].astype(jnp.bfloat16)

                    @pl.when(core == c)
                    def _():
                        own_ref[half, at[0], at[1]] = value

                    @pl.when(core != c)
                    def _():
                        other_ref[half, at[0], at[1]] = value


def projection_grads(place, x, d, depth, wide):
    part = 384
    out = jax.ShapeDtypeStruct((2, 4, 4, depth, wide), jnp.bfloat16)
    whole = pl.BlockSpec(out.shape, lambda i: (0, 0, 0, 0, 0))
    return pl.pallas_call(
        grads_kernel,
        grid=(x.shape[1] // part,),
        in_specs=[
            pl.BlockSpec(memory_space=pltpu.SMEM),
            pl.BlockSpec((x.shape[0], part), lambda i: (0, i)),
            pl.BlockSpec(d.shape, lambda i: (0, 0)),
        ],
        out_specs=[whole] * 2,
        out_shape=[out] * 2,
        scratch_shapes=[pltpu.VMEM((8 * depth, 4 * wide), jnp.float32)],
        cost_estimate=pl.CostEstimate(
            flops=2 * x.shape[0] * x.shape[1] * d.shape[1], bytes_accessed=2 * (x.size + d.size) + 4 * out.size, transcendentals=0
        ),
        compiler_params=pltpu.CompilerParams(vmem_limit_bytes=56 * 1024 * 1024),
        name="grads",
    )(place, x, d)


def cyclic_total(value, rest, name):
    size = len(rest) + 1
    every = jnp.concatenate([value] + rest)
    twice = jnp.concatenate([every, every])
    me = lax.axis_index(name)
    return jnp.sum(lax.dynamic_slice_in_dim(twice, (size - me) % size, size), 0, keepdims=True)


def rotary_tables():
    half = HEAD // 2
    places = np.arange(SEQ, dtype=np.float32)[:, None]
    freqs = np.float32(BASE) ** (-np.arange(half, dtype=np.float32) / np.float32(half))
    angles = places * freqs[None, :]
    cosine, sine = np.cos(angles), np.sin(angles)
    cosine = np.concatenate([cosine, cosine], 1)
    sine = np.concatenate([-sine, sine], 1)
    return jnp.asarray(cosine), jnp.asarray(sine)


def dot(a, b, dims):
    return lax.dot_general(a, b, (dims, ((), ())), preferred_element_type=jnp.float32)


def turned(v, cosine, sine):
    return (v * cosine + pltpu.roll(v, HEAD // 2, 1) * sine).astype(jnp.bfloat16)


def block_kernel(
    place_ref, x_ref, own_ref, other_ref, cot_ref, cos_ref, sin_ref, att_ref, dqkv_ref, dn_ref, gain_ref, w_ref, qkv_ref
):
    @pl.when(pl.program_id(0) == 0)
    def _():
        assemble(place_ref, own_ref, other_ref, w_ref)

    qkv_ref[...] = dot(x_ref[...], w_ref[...], ((1,), (0,)))
    cosine = jnp.concatenate([cos_ref[...]] * (SUB // SEQ), 0)
    sine = jnp.concatenate([sin_ref[...]] * (SUB // SEQ), 0)
    cosine2 = jnp.concatenate([cosine, cosine], 0)
    sine2 = jnp.concatenate([sine, sine], 0)
    row = lax.broadcasted_iota(jnp.int32, (2 * SUB, SUB), 0) % SUB
    col = lax.broadcasted_iota(jnp.int32, (2 * SUB, SUB), 1)
    seen = (col <= row) & (col // SEQ == row // SEQ)
    places = [(slice(t * SUB, (t + 1) * SUB), slice(2 * t, 2 * t + 2), s) for t in range(TILE // SUB) for s in range(2)]
    head = lambda s, n: slice((4 * s + n) * HEAD, (4 * s + n + 1) * HEAD)
    query = [
        turned(jnp.concatenate([qkv_ref[r, head(s, 0)], qkv_ref[r, head(s, 1)]], 0), cosine2, sine2) for r, _, s in places
    ]
    key = [turned(qkv_ref[r, head(s, 2)], cosine, sine) for r, _, s in places]
    value = [qkv_ref[r, head(s, 3)].astype(jnp.bfloat16) for r, _, s in places]
    scores = [dot(a, b, ((1,), (1,))) for a, b in zip(query, key)]
    cots = [cot_ref[s, p, 0].reshape(SUB, 2 * HEAD) for _, p, s in places]
    cots = [jnp.concatenate([a[:, :HEAD], a[:, HEAD:]], 0) for a in cots]
    d_probs = [dot(a, b, ((1,), (1,))) for a, b in zip(cots, value)]
    bent = [jnp.tanh(a * (FACTOR / CAP)) for a in scores]
    raised = [jnp.where(seen, jnp.exp(CAP * a), 0.0) for a in bent]
    sums = [jnp.sum(a, -1, keepdims=True) for a in raised]
    weights = [a / b for a, b in zip(raised, sums)]
    probs = [a.astype(jnp.bfloat16) for a in weights]
    att = [dot(a, b, ((1,), (0,))).astype(jnp.bfloat16) for a, b in zip(probs, value)]
    d_value = [dot(a, b, ((0,), (0,))).astype(jnp.bfloat16) for a, b in zip(probs, cots)]
    inner = [jnp.sum(a * b, -1, keepdims=True) for a, b in zip(weights, d_probs)]
    d_scores = [
        (a * (b - c) * (1.0 - d * d) * FACTOR).astype(jnp.bfloat16) for a, b, c, d in zip(weights, d_probs, inner, bent)
    ]
    d_query = [dot(a, b, ((1,), (0,))) for a, b in zip(d_scores, key)]
    d_key = [dot(a, b, ((0,), (0,))) for a, b in zip(d_scores, query)]
    for i, (r, p, s) in enumerate(places):
        for h in range(2):
            att_ref[s, p, :, h * HEAD : (h + 1) * HEAD] = att[i][h * SUB : (h + 1) * SUB].reshape(2, SEQ, HEAD)
        both = turned(d_query[i], cosine2, -sine2)
        dqkv_ref[r, head(s, 0)] = both[:SUB]
        dqkv_ref[r, head(s, 1)] = both[SUB:]
        dqkv_ref[r, head(s, 2)] = turned(d_key[i], cosine, -sine)
        dqkv_ref[r, head(s, 3)] = d_value[i]
    dn = dot(dqkv_ref[...], w_ref[...], ((1,), (1,)))
    dn_ref[...] = dn.astype(jnp.bfloat16)
    part = jnp.sum(dn * x_ref[...].astype(jnp.float32), 0, keepdims=True)

    @pl.when(pl.program_id(0) == 0)
    def _():
        gain_ref[...] = part

    @pl.when(pl.program_id(0) > 0)
    def _():
        gain_ref[...] += part


def block(place, x, own, other, cot, cosine, sine):
    rows, width = x.shape
    columns = 2 * own.shape[3]
    per = TILE // SEQ
    full = lambda shape: pl.BlockSpec(shape, lambda i: (0,) * len(shape))
    tile = lambda n: pl.BlockSpec((TILE, n), lambda i: (i, 0))
    flops = 4 * rows * width * columns + 12 * rows * SUB * columns
    return pl.pallas_call(
        block_kernel,
        grid=(rows // TILE,),
        in_specs=[
            pl.BlockSpec(memory_space=pltpu.SMEM),
            tile(width),
            full(own.shape),
            full(other.shape),
            pl.BlockSpec((2, per, 1, SEQ, 2 * HEAD), lambda i: (0, i, 0, 0, 0)),
            full((SEQ, HEAD)),
            full((SEQ, HEAD)),
        ],
        out_specs=[
            pl.BlockSpec((2, per, SEQ, 2 * HEAD), lambda i: (0, i, 0, 0)),
            tile(columns),
            tile(width),
            full((1, width)),
        ],
        out_shape=[
            jax.ShapeDtypeStruct((2, rows // SEQ, SEQ, 2 * HEAD), jnp.bfloat16),
            jax.ShapeDtypeStruct((rows, columns), jnp.bfloat16),
            jax.ShapeDtypeStruct((rows, width), jnp.bfloat16),
            jax.ShapeDtypeStruct((1, width), jnp.float32),
        ],
        scratch_shapes=[pltpu.VMEM((width, columns), jnp.bfloat16), pltpu.VMEM((TILE, columns), jnp.float32)],
        cost_estimate=pl.CostEstimate(
            flops=flops, bytes_accessed=2 * (2 * rows * width + width * columns + 3 * rows * columns), transcendentals=0
        ),
        compiler_params=pltpu.CompilerParams(vmem_limit_bytes=50 * 1024 * 1024),
        name="block",
    )(place, x, own, other, cot, cosine, sine)


def per_device(tokens, cotangent, pre_gain, w_query, key_weight, value_weight):
    c, x = lax.axis_index(CORE), lax.axis_index(XL)
    depth = w_query.shape[0]

    rows = tokens.astype(jnp.float32)
    inv_one = lax.rsqrt(jnp.mean(rows * rows, -1, keepdims=True) + EPS)
    unit_one = rows * inv_one
    gathered = lax.all_gather((unit_one * pre_gain).astype(jnp.bfloat16), Z, axis=0, tiled=True)

    place = jnp.stack([lax.axis_index(Y), lax.axis_index(X), c])
    plane = gather_plane(jnp.concatenate([w_query, key_weight, value_weight], 1))
    other = lax.ppermute(plane, CORE, SWAP)

    halves = cotangent.reshape(2, -1, cotangent.shape[1])
    own, got = pick(halves, x, 0), lax.ppermute(pick(halves, 1 - x, 0), XL, SWAP)
    cot = jnp.where(x == 0, jnp.stack([own, got]), jnp.stack([got, own]))
    cot = cot.reshape(2, -1, 1, SEQ, cot.shape[-1])

    cosine, sine = rotary_tables()
    att, joined, dn, gain = block(place, gathered, plane, other, cot, cosine, sine)
    scattered = lax.psum_scatter(dn, Z, scatter_dimension=0, tiled=True)

    att = att.reshape(2, -1, att.shape[-1])
    own, got = pick(att, x, 0), lax.ppermute(pick(att, 1 - x, 0), XL, SWAP)
    attended = jnp.where(x == 0, jnp.concatenate([own, got]), jnp.concatenate([got, own]))

    barrier = lax.optimization_barrier
    flip = lambda v, name, size, step: lax.ppermute(v, name, [(i, i ^ step) for i in range(size)])
    wide, few = w_query.shape[1], key_weight.shape[1]
    got = others([gain] * 4, X)
    own, other = projection_grads(place, gathered, joined, depth, wide)
    own, other, got = barrier((own, other, got))
    gain = cyclic_total(gain, got, X)
    moved, got = barrier((lax.ppermute(other, CORE, SWAP), others([gain] * 4, Y)))
    gain = cyclic_total(gain, got, Y)
    one, two = (narrow([own[h, r].astype(jnp.float32) + moved[h, r].astype(jnp.float32) for r in range(4)]) for h in range(2))
    one, two, gain = barrier((one, two, gain))
    moved_one, moved_two = others(one, X), others(two, Y)
    got = [flip(gain, Z, 8, 1), lax.ppermute(gain, CORE, SWAP), lax.ppermute(gain, (CORE, Z), [(i, i ^ 9) for i in range(16)])]
    moved_one, moved_two, got = barrier((moved_one, moved_two, got))
    gain = (gain + got[0]) + (got[1] + got[2])
    got = [flip(gain, Z, 8, step) for step in (2, 4, 6)]
    one, two = narrow(list(total(one[0], moved_one))), narrow(list(total(two[0], moved_two)))
    grad_query, grad_rest = total(one[0], others(one, Y)), total(two[0], others(two, X))
    grad_key, grad_value = grad_rest[:, :few], grad_rest[:, few:]
    gain = (gain + got[0]) + (got[1] + got[2])
    grad_pre = gain[0] / pre_gain

    d_normed = scattered.astype(jnp.float32)
    scaled = d_normed * pre_gain
    grad_tokens = inv_one * (scaled - unit_one * jnp.mean(scaled * unit_one, -1, keepdims=True))
    return (attended, grad_tokens.astype(jnp.bfloat16), grad_query, grad_key, grad_value, grad_pre)


def solution(mesh):
    torus = Mesh(mesh.devices.reshape(4, 2, 2, 2, 8), ALL)
    dp, tensor = (Y, XH, CORE), (XL, Z)
    in_specs = (P(ALL, None), P(dp, tensor), P(), P(dp, tensor), P(dp, tensor), P(dp, tensor))
    out_specs = (P(dp, tensor), P(ALL, None), P(dp, tensor), P(dp, tensor), P(dp, tensor), P())
    return jax.shard_map(per_device, mesh=torus, in_specs=in_specs, out_specs=out_specs, check_vma=False)
```

```python
import functools

import jax
import jax.numpy as jnp
import numpy as np
from jax import lax
from jax.experimental import pallas as pl
from jax.experimental.pallas import tpu as pltpu
from jax.sharding import Mesh
from jax.sharding import PartitionSpec as P

HEAD = 128
SEQ = 64
EPS = 1e-06
CAP = 50.0
BASE = 10000.0
FACTOR = 144.0**-0.5
TILE = 256
PART = 384
SUB = 128

Y, XH, CORE, XL, Z = "dp_0", "dp_1", "dp_2", "tensor_0", "tensor_1"
X = (XH, XL)
ALL = (Y, XH, CORE, XL, Z)
SWAP = [(0, 1), (1, 0)]


def shift(value, axis, size, step):
    return lax.ppermute(value, axis, [((i + step) % size, i) for i in range(size)])


def gather_plane(own, cot):
    row = jnp.stack([own] + [shift(own, X, 4, s) for s in (1, 2, 3)])
    row, cot = lax.optimization_barrier((row, cot))
    return jnp.stack([row] + [shift(row, Y, 4, s) for s in (1, 2, 3)]), cot


def pick(value, place, axis):
    return lax.dynamic_index_in_dim(value, place % value.shape[axis], axis, keepdims=False)


def others(terms, name):
    size = len(terms)
    return [shift(terms[size - s], name, size, s) for s in range(1, size)]


def total(first, rest):
    return sum((r.astype(jnp.float32) for r in rest), first.astype(jnp.float32))


def narrow(terms):
    return [terms[0]] + [t.astype(jnp.bfloat16) for t in terms[1:]]


def split_in_two(gain, wide):
    high = lax.reduce_precision(gain, 8, 7)
    low = lax.reduce_precision(gain - high, 8, 7)
    both = jnp.concatenate([high, low]).astype(jnp.bfloat16).reshape(-1, wide)
    return high + low, jnp.pad(both, ((0, -both.shape[0] % 8), (0, 0)))


def with_extra(terms, extra, name, width):
    shape, wide = terms[0].shape, terms[0].shape[-1]
    sent = [terms[0]] + [jnp.concatenate([t.astype(jnp.bfloat16).reshape(-1, wide), extra]) for t in terms[1:]]
    got = others(sent, name)
    rows = terms[0].size // wide
    used = 2 * width // wide
    gains = [jnp.sum(g[rows : rows + used].astype(jnp.float32).reshape(2, -1), 0, keepdims=True) for g in got]
    return [g[:rows].reshape(shape) for g in got], gains


def assemble(place_ref, own_ref, other_ref, w_ref):
    depth, wide = own_ref.shape[2:]
    y0, x0, core = place_ref[0], place_ref[1], place_ref[2]

    @pl.loop(0, 16)
    def _(i):
        dy, dx = i // 4, lax.rem(i, 4)
        y, x = lax.rem(y0 + dy, 4), lax.rem(x0 + dx, 4)
        col = pl.multiple_of(lax.rem(x, 2) * wide, 128)
        for ref, c in ((own_ref, core), (other_ref, 1 - core)):
            row = pl.multiple_of(((y * 2 + x // 2) * 2 + c) * depth, 16)
            w_ref[pl.ds(row, depth), pl.ds(col, wide)] = ref[dy, dx]


def grads_kernel(place_ref, x_ref, d_ref, own_ref, other_ref, dw_ref):
    depth, wide = own_ref.shape[3:]
    y0, x0, core = place_ref[0], place_ref[1], place_ref[2]
    step = pl.program_id(0)
    part = x_ref.shape[1]
    steps = dw_ref.shape[0] // part
    at = pl.ds(pl.multiple_of(lax.rem(step, steps) * part, part), part)
    dw_ref[at, :] = dot(x_ref[...], d_ref[...], ((0,), (0,)))

    @pl.when(lax.rem(step, steps) == steps - 1)
    def _():
        blocks = dw_ref.shape[0] // depth

        @pl.loop(0, blocks)
        def _(i):
            b = step // steps * blocks + i
            y, xh, c = b // 4, lax.rem(b // 2, 2), lax.rem(b, 2)
            rows = pl.ds(pl.multiple_of(i * depth, 16), depth)
            for xl in range(2):
                dy = lax.rem(y + 4 - y0, 4)
                dx = lax.rem(2 * xh + xl + 4 - x0, 4)
                for half, at in enumerate(((dx, dy), (dy, dx))):
                    col = (2 * xl + half) * wide
                    value = dw_ref[rows, col : col + wide].astype(jnp.bfloat16)

                    @pl.when(core == c)
                    def _():
                        own_ref[half, at[0], at[1]] = value

                    @pl.when(core != c)
                    def _():
                        other_ref[half, at[0], at[1]] = value


def projection_grads(place, x, d, depth, wide):
    part, width = PART, x.shape[1]
    out = jax.ShapeDtypeStruct((2, 4, 4, depth, wide), jnp.bfloat16)
    whole = pl.BlockSpec(out.shape, lambda i: (0, 0, 0, 0, 0))
    return pl.pallas_call(
        grads_kernel,
        grid=(width // part,),
        in_specs=[
            pl.BlockSpec(memory_space=pltpu.SMEM),
            pl.BlockSpec((x.shape[0], part), lambda i: (0, i)),
            pl.BlockSpec(d.shape, lambda i: (0, 0)),
        ],
        out_specs=[whole] * 2,
        out_shape=[out] * 2,
        scratch_shapes=[pltpu.VMEM((8 * depth, 4 * wide), jnp.float32)],
        cost_estimate=pl.CostEstimate(
            flops=2 * x.shape[0] * width * d.shape[1], bytes_accessed=2 * (x.size + d.size) + 4 * out.size, transcendentals=0
        ),
        compiler_params=pltpu.CompilerParams(vmem_limit_bytes=56 * 1024 * 1024),
        name="grads",
    )(place, x, d)


def cyclic_total(value, rest, name):
    size = len(rest) + 1
    every = jnp.concatenate([value] + rest)
    twice = jnp.concatenate([every, every])
    me = lax.axis_index(name)
    return jnp.sum(lax.dynamic_slice_in_dim(twice, (size - me) % size, size), 0, keepdims=True)


def rotary_tables():
    half = HEAD // 2
    places = np.arange(SEQ, dtype=np.float32)[:, None]
    freqs = np.float32(BASE) ** (-np.arange(half, dtype=np.float32) / np.float32(half))
    angles = places * freqs[None, :]
    cosine, sine = np.cos(angles), np.sin(angles)
    cosine = np.concatenate([cosine, cosine], 1)
    sine = np.concatenate([-sine, sine], 1)
    return jnp.asarray(cosine), jnp.asarray(sine)


def dot(a, b, dims):
    return lax.dot_general(a, b, (dims, ((), ())), preferred_element_type=jnp.float32)


def turned(v, cosine, sine):
    return (v * cosine + pltpu.roll(v, HEAD // 2, 1) * sine).astype(jnp.bfloat16)


def block_kernel(
    place_ref, x_ref, own_ref, other_ref, cot_ref, cot_got_ref, cos_ref, sin_ref,
    att_ref, att_sent_ref, dqkv_ref, dn_ref, gain_ref, w_ref, qkv_ref,
):
    @pl.when(pl.program_id(0) == 0)
    def _():
        assemble(place_ref, own_ref, other_ref, w_ref)

    qkv_ref[...] = dot(x_ref[...], w_ref[...], ((1,), (0,)))
    even = place_ref[3] == 0
    cosine = jnp.concatenate([cos_ref[...]] * (SUB // SEQ), 0)
    sine = jnp.concatenate([sin_ref[...]] * (SUB // SEQ), 0)
    cosine2 = jnp.concatenate([cosine, cosine], 0)
    sine2 = jnp.concatenate([sine, sine], 0)
    row = lax.broadcasted_iota(jnp.int32, (2 * SUB, SUB), 0) % SUB
    col = lax.broadcasted_iota(jnp.int32, (2 * SUB, SUB), 1)
    seen = (col <= row) & (col // SEQ == row // SEQ)
    places = [(slice(t * SUB, (t + 1) * SUB), slice(2 * t, 2 * t + 2), s) for t in range(TILE // SUB) for s in range(2)]
    head = lambda s, n: slice((4 * s + n) * HEAD, (4 * s + n + 1) * HEAD)
    query = [
        turned(jnp.concatenate([qkv_ref[r, head(s, 0)], qkv_ref[r, head(s, 1)]], 0), cosine2, sine2) for r, _, s in places
    ]
    key = [turned(qkv_ref[r, head(s, 2)], cosine, sine) for r, _, s in places]
    value = [qkv_ref[r, head(s, 3)].astype(jnp.bfloat16) for r, _, s in places]
    scores = [dot(a, b, ((1,), (1,))) for a, b in zip(query, key)]
    cots = [
        jnp.where(even, *[ref[p].reshape(SUB, 2 * HEAD) for ref in ((cot_ref, cot_got_ref), (cot_got_ref, cot_ref))[s]])
        for _, p, s in places
    ]
    cots = [jnp.concatenate([a[:, :HEAD], a[:, HEAD:]], 0) for a in cots]
    d_probs = [dot(a, b, ((1,), (1,))) for a, b in zip(cots, value)]
    bent = [jnp.tanh(a * (FACTOR / CAP)) for a in scores]
    raised = [jnp.where(seen, jnp.exp(CAP * a), 0.0) for a in bent]
    sums = [jnp.sum(a, -1, keepdims=True) for a in raised]
    weights = [a / b for a, b in zip(raised, sums)]
    probs = [a.astype(jnp.bfloat16) for a in weights]
    att = [dot(a, b, ((1,), (0,))).astype(jnp.bfloat16) for a, b in zip(probs, value)]
    d_value = [dot(a, b, ((0,), (0,))).astype(jnp.bfloat16) for a, b in zip(probs, cots)]
    inner = [jnp.sum(a * b, -1, keepdims=True) for a, b in zip(weights, d_probs)]
    d_scores = [
        (a * (b - c) * (1.0 - d * d) * FACTOR).astype(jnp.bfloat16) for a, b, c, d in zip(weights, d_probs, inner, bent)
    ]
    d_query = [dot(a, b, ((1,), (0,))) for a, b in zip(d_scores, key)]
    d_key = [dot(a, b, ((0,), (0,))) for a, b in zip(d_scores, query)]
    for i, (r, p, s) in enumerate(places):
        if s == 0:
            for h in range(2):
                first, second = (att[j][h * SUB : (h + 1) * SUB] for j in (i, i + 1))
                for ref, value in ((att_ref, (first, second)), (att_sent_ref, (second, first))):
                    ref[p, :, h * HEAD : (h + 1) * HEAD] = jnp.where(even, *value).reshape(2, SEQ, HEAD)
        both = turned(d_query[i], cosine2, -sine2)
        dqkv_ref[r, head(s, 0)] = both[:SUB]
        dqkv_ref[r, head(s, 1)] = both[SUB:]
        dqkv_ref[r, head(s, 2)] = turned(d_key[i], cosine, -sine)
        dqkv_ref[r, head(s, 3)] = d_value[i]

    @pl.when(pl.program_id(0) == 0)
    def _():
        gain_ref[...] = jnp.zeros_like(gain_ref)

    dn = dot(dqkv_ref[...], w_ref[...], ((1,), (1,)))
    dn_ref[...] = dn.astype(jnp.bfloat16)
    gain_ref[...] += jnp.sum(dn * x_ref[...].astype(jnp.float32), 0, keepdims=True)


def block(place, x, own, other, cot, cot_got, cosine, sine):
    rows, width = x.shape
    columns = 2 * own.shape[3]
    per = TILE // SEQ
    full = lambda shape: pl.BlockSpec(shape, lambda i: (0,) * len(shape))
    tile = lambda n: pl.BlockSpec((TILE, n), lambda i: (i, 0))
    heads = pl.BlockSpec((per, SEQ, 2 * HEAD), lambda i: (i, 0, 0))
    flops = 4 * rows * width * columns + 12 * rows * SUB * columns
    return pl.pallas_call(
        block_kernel,
        grid=(rows // TILE,),
        in_specs=[
            pl.BlockSpec(memory_space=pltpu.SMEM),
            tile(width),
            full(own.shape),
            full(other.shape),
            heads,
            heads,
            full((SEQ, HEAD)),
            full((SEQ, HEAD)),
        ],
        out_specs=[
            heads,
            heads,
            tile(columns),
            tile(width),
            full((1, width)),
        ],
        out_shape=[
            jax.ShapeDtypeStruct(cot.shape, jnp.bfloat16),
            jax.ShapeDtypeStruct(cot.shape, jnp.bfloat16),
            jax.ShapeDtypeStruct((rows, columns), jnp.bfloat16),
            jax.ShapeDtypeStruct((rows, width), jnp.bfloat16),
            jax.ShapeDtypeStruct((1, width), jnp.float32),
        ],
        scratch_shapes=[pltpu.VMEM((width, columns), jnp.bfloat16), pltpu.VMEM((TILE, columns), jnp.float32)],
        cost_estimate=pl.CostEstimate(
            flops=flops, bytes_accessed=2 * (2 * rows * width + width * columns + 3 * rows * columns), transcendentals=0
        ),
        compiler_params=pltpu.CompilerParams(vmem_limit_bytes=50 * 1024 * 1024),
        name="block",
    )(place, x, own, other, cot, cot_got, cosine, sine)


def per_device(tokens, cotangent, pre_gain, w_query, key_weight, value_weight):
    c, x = lax.axis_index(CORE), lax.axis_index(XL)
    depth = w_query.shape[0]

    rows = tokens.astype(jnp.float32)
    inv_one = lax.rsqrt(jnp.mean(rows * rows, -1, keepdims=True) + EPS)
    unit_one = rows * inv_one
    gathered = lax.all_gather((unit_one * pre_gain).astype(jnp.bfloat16), Z, axis=0, tiled=True)

    place = jnp.stack([lax.axis_index(Y), lax.axis_index(X), c, x])
    halves = cotangent.reshape(2, -1, cotangent.shape[1])
    got = lax.ppermute(pick(halves, 1 - x, 0), XL, SWAP)
    plane, got = gather_plane(jnp.concatenate([w_query, key_weight, value_weight], 1), got)
    other = lax.ppermute(plane, CORE, SWAP)

    in_heads = lambda v: v.reshape(-1, SEQ, v.shape[-1])
    own, got = in_heads(pick(halves, x, 0)), in_heads(got)
    cosine, sine = rotary_tables()
    att, sent, joined, dn, gain = block(place, gathered, plane, other, own, got, cosine, sine)
    scattered = lax.psum_scatter(dn, Z, scatter_dimension=0, tiled=True)

    back = lax.ppermute(sent, XL, SWAP)

    barrier = lax.optimization_barrier
    flip = lambda v, name, size, step: lax.ppermute(v, name, [(i, i ^ step) for i in range(size)])
    wide, few = w_query.shape[1], key_weight.shape[1]
    got = [flip(gain, Z, 8, step) for step in (2, 4, 6)]
    own, other = projection_grads(place, gathered, joined, depth, wide)
    own, other, got, back = barrier((own, other, got, back))
    gain = (gain + got[0]) + (got[1] + got[2])
    got = [flip(gain, Z, 8, 1), lax.ppermute(gain, CORE, SWAP), lax.ppermute(gain, (CORE, Z), [(i, i ^ 9) for i in range(16)])]
    moved, got = barrier((lax.ppermute(other, CORE, SWAP), got))
    gain = (gain + got[0]) + (got[1] + got[2])
    one, two = ([own[h, r].astype(jnp.float32) + moved[h, r].astype(jnp.float32) for r in range(4)] for h in range(2))
    mine, extra = split_in_two(gain, wide)
    got_one, gains = with_extra(one, extra, X, gain.shape[1])
    gain = cyclic_total(mine, gains, X)
    got_two = others(narrow(two), Y)
    one, two = list(total(one[0], got_one)), list(total(two[0], got_two))
    mine, extra = split_in_two(gain, wide)
    got_one, gains = with_extra(one, extra, Y, gain.shape[1])
    grad_pre = cyclic_total(mine, gains, Y)[0] / pre_gain
    grad_query, grad_rest = total(one[0], got_one), total(two[0], others(narrow(two), X))
    grad_key, grad_value = grad_rest[:, :few], grad_rest[:, few:]

    attended = jnp.zeros((2,) + att.shape, att.dtype)
    attended = lax.dynamic_update_index_in_dim(attended, att, x, 0)
    attended = lax.dynamic_update_index_in_dim(attended, back, 1 - x, 0).reshape(cotangent.shape)

    d_normed = scattered.astype(jnp.float32)
    scaled = d_normed * pre_gain
    grad_tokens = inv_one * (scaled - unit_one * jnp.mean(scaled * unit_one, -1, keepdims=True))
    return (attended, grad_tokens.astype(jnp.bfloat16), grad_query, grad_key, grad_value, grad_pre)


def solution(mesh):
    torus = Mesh(mesh.devices.reshape(4, 2, 2, 2, 8), ALL)
    dp, tensor = (Y, XH, CORE), (XL, Z)
    in_specs = (P(ALL, None), P(dp, tensor), P(), P(dp, tensor), P(dp, tensor), P(dp, tensor))
    out_specs = (P(dp, tensor), P(ALL, None), P(dp, tensor), P(dp, tensor), P(dp, tensor), P())
    return jax.shard_map(per_device, mesh=torus, in_specs=in_specs, out_specs=out_specs, check_vma=False)
```

```python
import functools

import jax
import jax.numpy as jnp
import numpy as np
from jax import lax
from jax.experimental import pallas as pl
from jax.experimental.pallas import tpu as pltpu
from jax.sharding import Mesh
from jax.sharding import PartitionSpec as P

HEAD = 128
SEQ = 64
EPS = 1e-06
CAP = 50.0
BASE = 10000.0
FACTOR = 144.0**-0.5
TILE = 256
PART = 384
SUB = 128

Y, XH, CORE, XL, Z = "dp_0", "dp_1", "dp_2", "tensor_0", "tensor_1"
X = (XH, XL)
ALL = (Y, XH, CORE, XL, Z)
SWAP = [(0, 1), (1, 0)]


def shift(value, axis, size, step):
    return lax.ppermute(value, axis, [((i + step) % size, i) for i in range(size)])


def gather_plane(own, cot):
    row = jnp.stack([own] + [shift(own, X, 4, s) for s in (1, 2, 3)])
    row, cot = lax.optimization_barrier((row, cot))
    return jnp.stack([row] + [shift(row, Y, 4, s) for s in (1, 2, 3)]), cot


def pick(value, place, axis):
    return lax.dynamic_index_in_dim(value, place % value.shape[axis], axis, keepdims=False)


def others(terms, name):
    size = len(terms)
    return [shift(terms[size - s], name, size, s) for s in range(1, size)]


def total(first, rest):
    return sum((r.astype(jnp.float32) for r in rest), first.astype(jnp.float32))


def narrow(terms):
    return [terms[0]] + [t.astype(jnp.bfloat16) for t in terms[1:]]


def split_in_two(gain, wide):
    high = lax.reduce_precision(gain, 8, 7)
    low = lax.reduce_precision(gain - high, 8, 7)
    both = jnp.concatenate([high, low]).astype(jnp.bfloat16).reshape(-1, wide)
    return high + low, jnp.pad(both, ((0, -both.shape[0] % 8), (0, 0)))


def with_extra(terms, extra, name, width):
    shape, wide = terms[0].shape, terms[0].shape[-1]
    sent = [terms[0]] + [jnp.concatenate([t.astype(jnp.bfloat16).reshape(-1, wide), extra]) for t in terms[1:]]
    got = others(sent, name)
    rows = terms[0].size // wide
    used = 2 * width // wide
    gains = [jnp.sum(g[rows : rows + used].astype(jnp.float32).reshape(2, -1), 0, keepdims=True) for g in got]
    return [g[:rows].reshape(shape) for g in got], gains


def assemble(place_ref, own_ref, other_ref, w_ref):
    depth, wide = own_ref.shape[2:]
    y0, x0, core = place_ref[0], place_ref[1], place_ref[2]

    @pl.loop(0, 16)
    def _(i):
        dy, dx = i // 4, lax.rem(i, 4)
        y, x = lax.rem(y0 + dy, 4), lax.rem(x0 + dx, 4)
        col = pl.multiple_of(lax.rem(x, 2) * wide, 128)
        for ref, c in ((own_ref, core), (other_ref, 1 - core)):
            row = pl.multiple_of(((y * 2 + x // 2) * 2 + c) * depth, 16)
            w_ref[pl.ds(row, depth), pl.ds(col, wide)] = ref[dy, dx]


def grads_kernel(place_ref, x_ref, d_ref, own_ref, other_ref, dw_ref):
    depth, wide = own_ref.shape[3:]
    y0, x0, core = place_ref[0], place_ref[1], place_ref[2]
    step = pl.program_id(0)
    part = x_ref.shape[1]
    steps = dw_ref.shape[0] // part
    at = pl.ds(pl.multiple_of(lax.rem(step, steps) * part, part), part)
    dw_ref[at, :] = dot(x_ref[...], d_ref[...], ((0,), (0,)))

    @pl.when(lax.rem(step, steps) == steps - 1)
    def _():
        blocks = dw_ref.shape[0] // depth

        @pl.loop(0, blocks)
        def _(i):
            b = step // steps * blocks + i
            y, xh, c = b // 4, lax.rem(b // 2, 2), lax.rem(b, 2)
            rows = pl.ds(pl.multiple_of(i * depth, 16), depth)
            for xl in range(2):
                dy = lax.rem(y + 4 - y0, 4)
                dx = lax.rem(2 * xh + xl + 4 - x0, 4)
                for half, at in enumerate(((dx, dy), (dy, dx))):
                    col = (2 * xl + half) * wide
                    value = dw_ref[rows, col : col + wide].astype(jnp.bfloat16)

                    @pl.when(core == c)
                    def _():
                        own_ref[half, at[0], at[1]] = value

                    @pl.when(core != c)
                    def _():
                        other_ref[half, at[0], at[1]] = value


def projection_grads(place, x, d, depth, wide):
    part, width = PART, x.shape[1]
    out = jax.ShapeDtypeStruct((2, 4, 4, depth, wide), jnp.bfloat16)
    whole = pl.BlockSpec(out.shape, lambda i: (0, 0, 0, 0, 0))
    return pl.pallas_call(
        grads_kernel,
        grid=(width // part,),
        in_specs=[
            pl.BlockSpec(memory_space=pltpu.SMEM),
            pl.BlockSpec((x.shape[0], part), lambda i: (0, i)),
            pl.BlockSpec(d.shape, lambda i: (0, 0)),
        ],
        out_specs=[whole] * 2,
        out_shape=[out] * 2,
        scratch_shapes=[pltpu.VMEM((8 * depth, 4 * wide), jnp.float32)],
        cost_estimate=pl.CostEstimate(
            flops=2 * x.shape[0] * width * d.shape[1], bytes_accessed=2 * (x.size + d.size) + 4 * out.size, transcendentals=0
        ),
        compiler_params=pltpu.CompilerParams(vmem_limit_bytes=56 * 1024 * 1024),
        name="grads",
    )(place, x, d)


def cyclic_total(value, rest, name):
    size = len(rest) + 1
    every = jnp.concatenate([value] + rest)
    twice = jnp.concatenate([every, every])
    me = lax.axis_index(name)
    return jnp.sum(lax.dynamic_slice_in_dim(twice, (size - me) % size, size), 0, keepdims=True)


def rotary_tables():
    half = HEAD // 2
    places = np.arange(SEQ, dtype=np.float32)[:, None]
    freqs = np.float32(BASE) ** (-np.arange(half, dtype=np.float32) / np.float32(half))
    angles = places * freqs[None, :]
    cosine, sine = np.cos(angles), np.sin(angles)
    cosine = np.concatenate([cosine, cosine], 1)
    sine = np.concatenate([-sine, sine], 1)
    return jnp.asarray(cosine), jnp.asarray(sine)


def dot(a, b, dims):
    return lax.dot_general(a, b, (dims, ((), ())), preferred_element_type=jnp.float32)


def turned(v, cosine, sine):
    return (v * cosine + pltpu.roll(v, HEAD // 2, 1) * sine).astype(jnp.bfloat16)


def block_kernel(
    place_ref, x_ref, own_ref, other_ref, cot_ref, cot_got_ref, cos_ref, sin_ref,
    att_ref, att_sent_ref, dqkv_ref, dn_ref, gain_ref, w_ref, qkv_ref,
):
    @pl.when(pl.program_id(0) == 0)
    def _():
        assemble(place_ref, own_ref, other_ref, w_ref)

    qkv_ref[...] = dot(x_ref[...], w_ref[...], ((1,), (0,)))
    even = place_ref[3] == 0
    cosine = jnp.concatenate([cos_ref[...]] * (SUB // SEQ), 0)
    sine = jnp.concatenate([sin_ref[...]] * (SUB // SEQ), 0)
    cosine2 = jnp.concatenate([cosine, cosine], 0)
    sine2 = jnp.concatenate([sine, sine], 0)
    row = lax.broadcasted_iota(jnp.int32, (2 * SUB, SUB), 0) % SUB
    col = lax.broadcasted_iota(jnp.int32, (2 * SUB, SUB), 1)
    seen = (col <= row) & (col // SEQ == row // SEQ)
    places = [(slice(t * SUB, (t + 1) * SUB), slice(2 * t, 2 * t + 2), s) for t in range(TILE // SUB) for s in range(2)]
    head = lambda s, n: slice((4 * s + n) * HEAD, (4 * s + n + 1) * HEAD)
    query = [
        turned(jnp.concatenate([qkv_ref[r, head(s, 0)], qkv_ref[r, head(s, 1)]], 0), cosine2, sine2) for r, _, s in places
    ]
    key = [turned(qkv_ref[r, head(s, 2)], cosine, sine) for r, _, s in places]
    value = [qkv_ref[r, head(s, 3)].astype(jnp.bfloat16) for r, _, s in places]
    scores = [dot(a, b, ((1,), (1,))) for a, b in zip(query, key)]
    cots = [
        jnp.where(even, *[ref[p].reshape(SUB, 2 * HEAD) for ref in ((cot_ref, cot_got_ref), (cot_got_ref, cot_ref))[s]])
        for _, p, s in places
    ]
    cots = [jnp.concatenate([a[:, :HEAD], a[:, HEAD:]], 0) for a in cots]
    d_probs = [dot(a, b, ((1,), (1,))) for a, b in zip(cots, value)]
    bent = [jnp.tanh(a * (FACTOR / CAP)) for a in scores]
    raised = [jnp.where(seen, jnp.exp(CAP * a), 0.0) for a in bent]
    sums = [jnp.sum(a, -1, keepdims=True) for a in raised]
    weights = [a / b for a, b in zip(raised, sums)]
    probs = [a.astype(jnp.bfloat16) for a in weights]
    att = [dot(a, b, ((1,), (0,))).astype(jnp.bfloat16) for a, b in zip(probs, value)]
    d_value = [dot(a, b, ((0,), (0,))).astype(jnp.bfloat16) for a, b in zip(probs, cots)]
    inner = [jnp.sum(a * b, -1, keepdims=True) for a, b in zip(weights, d_probs)]
    d_scores = [
        (a * (b - c) * (1.0 - d * d) * FACTOR).astype(jnp.bfloat16) for a, b, c, d in zip(weights, d_probs, inner, bent)
    ]
    d_query = [dot(a, b, ((1,), (0,))) for a, b in zip(d_scores, key)]
    d_key = [dot(a, b, ((0,), (0,))) for a, b in zip(d_scores, query)]
    for i, (r, p, s) in enumerate(places):
        if s == 0:
            for h in range(2):
                first, second = (att[j][h * SUB : (h + 1) * SUB] for j in (i, i + 1))
                for ref, value in ((att_ref, (first, second)), (att_sent_ref, (second, first))):
                    ref[p, :, h * HEAD : (h + 1) * HEAD] = jnp.where(even, *value).reshape(2, SEQ, HEAD)
        both = turned(d_query[i], cosine2, -sine2)
        dqkv_ref[r, head(s, 0)] = both[:SUB]
        dqkv_ref[r, head(s, 1)] = both[SUB:]
        dqkv_ref[r, head(s, 2)] = turned(d_key[i], cosine, -sine)
        dqkv_ref[r, head(s, 3)] = d_value[i]

    @pl.when(pl.program_id(0) == 0)
    def _():
        gain_ref[...] = jnp.zeros_like(gain_ref)

    dn = dot(dqkv_ref[...], w_ref[...], ((1,), (1,)))
    dn_ref[...] = dn.astype(jnp.bfloat16)
    gain_ref[...] += jnp.sum(dn * x_ref[...].astype(jnp.float32), 0, keepdims=True)


def block(place, x, own, other, cot, cot_got, cosine, sine):
    rows, width = x.shape
    columns = 2 * own.shape[3]
    per = TILE // SEQ
    full = lambda shape: pl.BlockSpec(shape, lambda i: (0,) * len(shape))
    tile = lambda n: pl.BlockSpec((TILE, n), lambda i: (i, 0))
    heads = pl.BlockSpec((per, SEQ, 2 * HEAD), lambda i: (i, 0, 0))
    flops = 4 * rows * width * columns + 12 * rows * SUB * columns
    return pl.pallas_call(
        block_kernel,
        grid=(rows // TILE,),
        in_specs=[
            pl.BlockSpec(memory_space=pltpu.SMEM),
            tile(width),
            full(own.shape),
            full(other.shape),
            heads,
            heads,
            full((SEQ, HEAD)),
            full((SEQ, HEAD)),
        ],
        out_specs=[
            heads,
            heads,
            tile(columns),
            tile(width),
            full((1, width)),
        ],
        out_shape=[
            jax.ShapeDtypeStruct(cot.shape, jnp.bfloat16),
            jax.ShapeDtypeStruct(cot.shape, jnp.bfloat16),
            jax.ShapeDtypeStruct((rows, columns), jnp.bfloat16),
            jax.ShapeDtypeStruct((rows, width), jnp.bfloat16),
            jax.ShapeDtypeStruct((1, width), jnp.float32),
        ],
        scratch_shapes=[pltpu.VMEM((width, columns), jnp.bfloat16), pltpu.VMEM((TILE, columns), jnp.float32)],
        cost_estimate=pl.CostEstimate(
            flops=flops, bytes_accessed=2 * (2 * rows * width + width * columns + 3 * rows * columns), transcendentals=0
        ),
        compiler_params=pltpu.CompilerParams(vmem_limit_bytes=50 * 1024 * 1024),
        name="block",
    )(place, x, own, other, cot, cot_got, cosine, sine)


def norm_kernel(tokens_ref, gain_ref, normed_ref, inverse_ref):
    rows = tokens_ref[...].astype(jnp.float32)
    inverse = lax.rsqrt(jnp.mean(rows * rows, -1, keepdims=True) + EPS)
    normed_ref[...] = (rows * inverse * gain_ref[...]).astype(jnp.bfloat16)
    inverse_ref[...] = inverse


def norm_back_kernel(d_ref, tokens_ref, inverse_ref, gain_ref, out_ref):
    inverse = inverse_ref[...]
    unit = tokens_ref[...].astype(jnp.float32) * inverse
    scaled = d_ref[...].astype(jnp.float32) * gain_ref[...]
    out_ref[...] = (inverse * (scaled - unit * jnp.mean(scaled * unit, -1, keepdims=True))).astype(jnp.bfloat16)


def by_rows(kernel, name, outs, args):
    spec = lambda a: pl.BlockSpec((64, a.shape[1]), lambda i: (i, 0)) if a.shape[0] > 1 else pl.BlockSpec(a.shape, lambda i: (0, 0))
    return pl.pallas_call(
        kernel,
        grid=(args[0].shape[0] // 64,),
        in_specs=[spec(a) for a in args],
        out_specs=[spec(o) for o in outs],
        out_shape=outs,
        compiler_params=pltpu.CompilerParams(vmem_limit_bytes=60 * 1024 * 1024),
        name=name,
    )(*args)


def per_device(tokens, cotangent, pre_gain, w_query, key_weight, value_weight):
    c, x = lax.axis_index(CORE), lax.axis_index(XL)
    depth = w_query.shape[0]

    gain_row = pre_gain[None]
    like = lambda width, kind: jax.ShapeDtypeStruct((tokens.shape[0], width), kind)
    normed, inverse = by_rows(
        norm_kernel, "norm", [like(tokens.shape[1], jnp.bfloat16), like(1, jnp.float32)], (tokens, gain_row)
    )
    gathered = lax.all_gather(normed, Z, axis=0, tiled=True)

    place = jnp.stack([lax.axis_index(Y), lax.axis_index(X), c, x])
    halves = cotangent.reshape(2, -1, cotangent.shape[1])
    got = lax.ppermute(pick(halves, 1 - x, 0), XL, SWAP)
    plane, got = gather_plane(jnp.concatenate([w_query, key_weight, value_weight], 1), got)
    other = lax.ppermute(plane, CORE, SWAP)

    in_heads = lambda v: v.reshape(-1, SEQ, v.shape[-1])
    own, got = in_heads(pick(halves, x, 0)), in_heads(got)
    cosine, sine = rotary_tables()
    att, sent, joined, dn, gain = block(place, gathered, plane, other, own, got, cosine, sine)
    scattered = lax.psum_scatter(dn, Z, scatter_dimension=0, tiled=True)

    back = lax.ppermute(sent, XL, SWAP)

    barrier = lax.optimization_barrier
    flip = lambda v, name, size, step: lax.ppermute(v, name, [(i, i ^ step) for i in range(size)])
    wide, few = w_query.shape[1], key_weight.shape[1]
    got = [flip(gain, Z, 8, step) for step in (2, 4, 6)]
    own, other = projection_grads(place, gathered, joined, depth, wide)
    own, other, got, back = barrier((own, other, got, back))
    gain = (gain + got[0]) + (got[1] + got[2])
    got = [flip(gain, Z, 8, 1), lax.ppermute(gain, CORE, SWAP), lax.ppermute(gain, (CORE, Z), [(i, i ^ 9) for i in range(16)])]
    moved, got = barrier((lax.ppermute(other, CORE, SWAP), got))
    gain = (gain + got[0]) + (got[1] + got[2])
    one, two = ([own[h, r].astype(jnp.float32) + moved[h, r].astype(jnp.float32) for r in range(4)] for h in range(2))
    mine, extra = split_in_two(gain, wide)
    got_one, gains = with_extra(one, extra, X, gain.shape[1])
    gain = cyclic_total(mine, gains, X)
    got_two = others(narrow(two), Y)
    one, two = list(total(one[0], got_one)), list(total(two[0], got_two))
    mine, extra = split_in_two(gain, wide)
    got_one, gains = with_extra(one, extra, Y, gain.shape[1])
    got_two = others(narrow(two), X)
    (grad_tokens,) = by_rows(
        norm_back_kernel, "norm_back", [like(tokens.shape[1], jnp.bfloat16)], (scattered, tokens, inverse, gain_row)
    )
    got_one, gains, got_two, grad_tokens = barrier((got_one, gains, got_two, grad_tokens))
    grad_pre = cyclic_total(mine, gains, Y)[0] / pre_gain
    grad_query, grad_rest = total(one[0], got_one), total(two[0], got_two)
    grad_key, grad_value = grad_rest[:, :few], grad_rest[:, few:]

    attended = jnp.zeros((2,) + att.shape, att.dtype)
    attended = lax.dynamic_update_index_in_dim(attended, att, x, 0)
    attended = lax.dynamic_update_index_in_dim(attended, back, 1 - x, 0).reshape(cotangent.shape)

    return (attended, grad_tokens, grad_query, grad_key, grad_value, grad_pre)


def solution(mesh):
    torus = Mesh(mesh.devices.reshape(4, 2, 2, 2, 8), ALL)
    dp, tensor = (Y, XH, CORE), (XL, Z)
    in_specs = (P(ALL, None), P(dp, tensor), P(), P(dp, tensor), P(dp, tensor), P(dp, tensor))
    out_specs = (P(dp, tensor), P(ALL, None), P(dp, tensor), P(dp, tensor), P(dp, tensor), P())
    return jax.shard_map(per_device, mesh=torus, in_specs=in_specs, out_specs=out_specs, check_vma=False)
```

```python
import functools

import jax
import jax.numpy as jnp
import numpy as np
from jax import lax
from jax.experimental import pallas as pl
from jax.experimental.pallas import tpu as pltpu
from jax.sharding import Mesh
from jax.sharding import PartitionSpec as P

HEAD = 128
SEQ = 64
EPS = 1e-06
CAP = 50.0
BASE = 10000.0
FACTOR = 144.0**-0.5
TILE = 256
PART = 1152
SUB = 128

Y, XH, CORE, XL, Z = "dp_0", "dp_1", "dp_2", "tensor_0", "tensor_1"
X = (XH, XL)
ALL = (Y, XH, CORE, XL, Z)
SWAP = [(0, 1), (1, 0)]


def shift(value, axis, size, step):
    return lax.ppermute(value, axis, [((i + step) % size, i) for i in range(size)])


def gather_plane(own, cot):
    row = jnp.stack([own] + [shift(own, X, 4, s) for s in (1, 2, 3)])
    row, cot = lax.optimization_barrier((row, cot))
    return jnp.stack([row] + [shift(row, Y, 4, s) for s in (1, 2, 3)]), cot


def pick(value, place, axis):
    return lax.dynamic_index_in_dim(value, place % value.shape[axis], axis, keepdims=False)


def others(terms, name):
    size = len(terms)
    return [shift(terms[size - s], name, size, s) for s in range(1, size)]


def total(first, rest):
    return sum((r.astype(jnp.float32) for r in rest), first.astype(jnp.float32))


def narrow(terms):
    return [terms[0]] + [t.astype(jnp.bfloat16) for t in terms[1:]]


def split_in_two(gain, wide):
    high = lax.reduce_precision(gain, 8, 7)
    low = lax.reduce_precision(gain - high, 8, 7)
    both = jnp.concatenate([high, low]).astype(jnp.bfloat16).reshape(-1, wide)
    return high + low, jnp.pad(both, ((0, -both.shape[0] % 8), (0, 0)))


def with_extra(terms, extra, name, width):
    shape, wide = terms[0].shape, terms[0].shape[-1]
    sent = [terms[0]] + [jnp.concatenate([t.astype(jnp.bfloat16).reshape(-1, wide), extra]) for t in terms[1:]]
    got = others(sent, name)
    rows = terms[0].size // wide
    used = 2 * width // wide
    gains = [jnp.sum(g[rows : rows + used].astype(jnp.float32).reshape(2, -1), 0, keepdims=True) for g in got]
    return [g[:rows].reshape(shape) for g in got], gains


def assemble(place_ref, own_ref, other_ref, w_ref):
    depth, wide = own_ref.shape[2:]
    y0, x0, core = place_ref[0], place_ref[1], place_ref[2]

    @pl.loop(0, 16)
    def _(i):
        dy, dx = i // 4, lax.rem(i, 4)
        y, x = lax.rem(y0 + dy, 4), lax.rem(x0 + dx, 4)
        col = pl.multiple_of(lax.rem(x, 2) * wide, 128)
        for ref, c in ((own_ref, core), (other_ref, 1 - core)):
            row = pl.multiple_of(((y * 2 + x // 2) * 2 + c) * depth, 16)
            w_ref[pl.ds(row, depth), pl.ds(col, wide)] = ref[dy, dx]


def grads_kernel(place_ref, x_ref, d_ref, own_ref, other_ref, dw_ref):
    depth, wide = own_ref.shape[3:]
    y0, x0, core = place_ref[0], place_ref[1], place_ref[2]
    step = pl.program_id(0)
    part = x_ref.shape[1]
    steps = dw_ref.shape[0] // part
    at = pl.ds(pl.multiple_of(lax.rem(step, steps) * part, part), part)
    dw_ref[at, :] = dot(x_ref[...], d_ref[...], ((0,), (0,)))

    @pl.when(lax.rem(step, steps) == steps - 1)
    def _():
        blocks = dw_ref.shape[0] // depth

        @pl.loop(0, blocks)
        def _(i):
            b = step // steps * blocks + i
            y, xh, c = b // 4, lax.rem(b // 2, 2), lax.rem(b, 2)
            rows = pl.ds(pl.multiple_of(i * depth, 16), depth)
            for xl in range(2):
                dy = lax.rem(y + 4 - y0, 4)
                dx = lax.rem(2 * xh + xl + 4 - x0, 4)
                for half, at in enumerate(((dx, dy), (dy, dx))):
                    col = (2 * xl + half) * wide
                    value = dw_ref[rows, col : col + wide].astype(jnp.bfloat16)

                    @pl.when(core == c)
                    def _():
                        own_ref[half, at[0], at[1]] = value

                    @pl.when(core != c)
                    def _():
                        other_ref[half, at[0], at[1]] = value


def projection_grads(place, x, d, depth, wide):
    part, width = PART, x.shape[1]
    out = jax.ShapeDtypeStruct((2, 4, 4, depth, wide), jnp.bfloat16)
    whole = pl.BlockSpec(out.shape, lambda i: (0, 0, 0, 0, 0))
    return pl.pallas_call(
        grads_kernel,
        grid=(width // part,),
        in_specs=[
            pl.BlockSpec(memory_space=pltpu.SMEM),
            pl.BlockSpec((x.shape[0], part), lambda i: (0, i)),
            pl.BlockSpec(d.shape, lambda i: (0, 0)),
        ],
        out_specs=[whole] * 2,
        out_shape=[out] * 2,
        scratch_shapes=[pltpu.VMEM((8 * depth, 4 * wide), jnp.float32)],
        cost_estimate=pl.CostEstimate(
            flops=2 * x.shape[0] * width * d.shape[1], bytes_accessed=2 * (x.size + d.size) + 4 * out.size, transcendentals=0
        ),
        compiler_params=pltpu.CompilerParams(vmem_limit_bytes=56 * 1024 * 1024),
        name="grads",
    )(place, x, d)


def cyclic_total(value, rest, name):
    size = len(rest) + 1
    every = jnp.concatenate([value] + rest)
    twice = jnp.concatenate([every, every])
    me = lax.axis_index(name)
    return jnp.sum(lax.dynamic_slice_in_dim(twice, (size - me) % size, size), 0, keepdims=True)


def rotary_tables():
    half = HEAD // 2
    places = np.arange(SEQ, dtype=np.float32)[:, None]
    freqs = np.float32(BASE) ** (-np.arange(half, dtype=np.float32) / np.float32(half))
    angles = places * freqs[None, :]
    cosine, sine = np.cos(angles), np.sin(angles)
    cosine = np.concatenate([cosine, cosine], 1)
    sine = np.concatenate([-sine, sine], 1)
    return jnp.asarray(cosine), jnp.asarray(sine)


def dot(a, b, dims):
    return lax.dot_general(a, b, (dims, ((), ())), preferred_element_type=jnp.float32)


def turned(v, cosine, sine):
    return (v * cosine + pltpu.roll(v, HEAD // 2, 1) * sine).astype(jnp.bfloat16)


def block_kernel(
    place_ref, x_ref, own_ref, other_ref, cot_ref, cot_got_ref, cos_ref, sin_ref,
    att_ref, att_sent_ref, dqkv_ref, dn_ref, gain_ref, w_ref, qkv_ref,
):
    @pl.when(pl.program_id(0) == 0)
    def _():
        assemble(place_ref, own_ref, other_ref, w_ref)

    qkv_ref[...] = dot(x_ref[...], w_ref[...], ((1,), (0,)))
    even = place_ref[3] == 0
    cosine = jnp.concatenate([cos_ref[...]] * (SUB // SEQ), 0)
    sine = jnp.concatenate([sin_ref[...]] * (SUB // SEQ), 0)
    cosine2 = jnp.concatenate([cosine, cosine], 0)
    sine2 = jnp.concatenate([sine, sine], 0)
    row = lax.broadcasted_iota(jnp.int32, (2 * SUB, SUB), 0) % SUB
    col = lax.broadcasted_iota(jnp.int32, (2 * SUB, SUB), 1)
    seen = (col <= row) & (col // SEQ == row // SEQ)
    places = [(slice(t * SUB, (t + 1) * SUB), slice(2 * t, 2 * t + 2), s) for t in range(TILE // SUB) for s in range(2)]
    head = lambda s, n: slice((4 * s + n) * HEAD, (4 * s + n + 1) * HEAD)
    query = [
        turned(jnp.concatenate([qkv_ref[r, head(s, 0)], qkv_ref[r, head(s, 1)]], 0), cosine2, sine2) for r, _, s in places
    ]
    key = [turned(qkv_ref[r, head(s, 2)], cosine, sine) for r, _, s in places]
    value = [qkv_ref[r, head(s, 3)].astype(jnp.bfloat16) for r, _, s in places]
    scores = [dot(a, b, ((1,), (1,))) for a, b in zip(query, key)]
    cots = [
        jnp.where(even, *[ref[p].reshape(SUB, 2 * HEAD) for ref in ((cot_ref, cot_got_ref), (cot_got_ref, cot_ref))[s]])
        for _, p, s in places
    ]
    cots = [jnp.concatenate([a[:, :HEAD], a[:, HEAD:]], 0) for a in cots]
    d_probs = [dot(a, b, ((1,), (1,))) for a, b in zip(cots, value)]
    bent = [jnp.tanh(a * (FACTOR / CAP)) for a in scores]
    raised = [jnp.where(seen, jnp.exp(CAP * a), 0.0) for a in bent]
    sums = [jnp.sum(a, -1, keepdims=True) for a in raised]
    weights = [a / b for a, b in zip(raised, sums)]
    probs = [a.astype(jnp.bfloat16) for a in weights]
    att = [dot(a, b, ((1,), (0,))).astype(jnp.bfloat16) for a, b in zip(probs, value)]
    d_value = [dot(a, b, ((0,), (0,))).astype(jnp.bfloat16) for a, b in zip(probs, cots)]
    inner = [jnp.sum(a * b, -1, keepdims=True) for a, b in zip(weights, d_probs)]
    d_scores = [
        (a * (b - c) * (1.0 - d * d) * FACTOR).astype(jnp.bfloat16) for a, b, c, d in zip(weights, d_probs, inner, bent)
    ]
    d_query = [dot(a, b, ((1,), (0,))) for a, b in zip(d_scores, key)]
    d_key = [dot(a, b, ((0,), (0,))) for a, b in zip(d_scores, query)]
    for i, (r, p, s) in enumerate(places):
        if s == 0:
            for h in range(2):
                first, second = (att[j][h * SUB : (h + 1) * SUB] for j in (i, i + 1))
                for ref, value in ((att_ref, (first, second)), (att_sent_ref, (second, first))):
                    ref[p, :, h * HEAD : (h + 1) * HEAD] = jnp.where(even, *value).reshape(2, SEQ, HEAD)
        both = turned(d_query[i], cosine2, -sine2)
        dqkv_ref[r, head(s, 0)] = both[:SUB]
        dqkv_ref[r, head(s, 1)] = both[SUB:]
        dqkv_ref[r, head(s, 2)] = turned(d_key[i], cosine, -sine)
        dqkv_ref[r, head(s, 3)] = d_value[i]

    @pl.when(pl.program_id(0) == 0)
    def _():
        gain_ref[...] = jnp.zeros_like(gain_ref)

    dn = dot(dqkv_ref[...], w_ref[...], ((1,), (1,)))
    dn_ref[...] = dn.astype(jnp.bfloat16)
    gain_ref[...] += jnp.sum(dn * x_ref[...].astype(jnp.float32), 0, keepdims=True)


def block(place, x, own, other, cot, cot_got, cosine, sine):
    rows, width = x.shape
    columns = 2 * own.shape[3]
    per = TILE // SEQ
    full = lambda shape: pl.BlockSpec(shape, lambda i: (0,) * len(shape))
    tile = lambda n: pl.BlockSpec((TILE, n), lambda i: (i, 0))
    heads = pl.BlockSpec((per, SEQ, 2 * HEAD), lambda i: (i, 0, 0))
    flops = 4 * rows * width * columns + 12 * rows * SUB * columns
    return pl.pallas_call(
        block_kernel,
        grid=(rows // TILE,),
        in_specs=[
            pl.BlockSpec(memory_space=pltpu.SMEM),
            tile(width),
            full(own.shape),
            full(other.shape),
            heads,
            heads,
            full((SEQ, HEAD)),
            full((SEQ, HEAD)),
        ],
        out_specs=[
            heads,
            heads,
            tile(columns),
            tile(width),
            full((1, width)),
        ],
        out_shape=[
            jax.ShapeDtypeStruct(cot.shape, jnp.bfloat16),
            jax.ShapeDtypeStruct(cot.shape, jnp.bfloat16),
            jax.ShapeDtypeStruct((rows, columns), jnp.bfloat16),
            jax.ShapeDtypeStruct((rows, width), jnp.bfloat16),
            jax.ShapeDtypeStruct((1, width), jnp.float32),
        ],
        scratch_shapes=[pltpu.VMEM((width, columns), jnp.bfloat16), pltpu.VMEM((TILE, columns), jnp.float32)],
        cost_estimate=pl.CostEstimate(
            flops=flops, bytes_accessed=2 * (2 * rows * width + width * columns + 3 * rows * columns), transcendentals=0
        ),
        compiler_params=pltpu.CompilerParams(vmem_limit_bytes=50 * 1024 * 1024),
        name="block",
    )(place, x, own, other, cot, cot_got, cosine, sine)


def norm_kernel(tokens_ref, gain_ref, normed_ref, inverse_ref):
    rows = tokens_ref[...].astype(jnp.float32)
    inverse = lax.rsqrt(jnp.mean(rows * rows, -1, keepdims=True) + EPS)
    normed_ref[...] = (rows * inverse * gain_ref[...]).astype(jnp.bfloat16)
    inverse_ref[...] = inverse


def norm_back_kernel(d_ref, tokens_ref, inverse_ref, gain_ref, out_ref):
    inverse = inverse_ref[...]
    unit = tokens_ref[...].astype(jnp.float32) * inverse
    scaled = d_ref[...].astype(jnp.float32) * gain_ref[...]
    out_ref[...] = (inverse * (scaled - unit * jnp.mean(scaled * unit, -1, keepdims=True))).astype(jnp.bfloat16)


def by_rows(kernel, name, outs, args):
    spec = lambda a: pl.BlockSpec((64, a.shape[1]), lambda i: (i, 0)) if a.shape[0] > 1 else pl.BlockSpec(a.shape, lambda i: (0, 0))
    return pl.pallas_call(
        kernel,
        grid=(args[0].shape[0] // 64,),
        in_specs=[spec(a) for a in args],
        out_specs=[spec(o) for o in outs],
        out_shape=outs,
        compiler_params=pltpu.CompilerParams(vmem_limit_bytes=60 * 1024 * 1024),
        name=name,
    )(*args)


def per_device(tokens, cotangent, pre_gain, w_query, key_weight, value_weight):
    c, x = lax.axis_index(CORE), lax.axis_index(XL)
    depth = w_query.shape[0]

    gain_row = pre_gain[None]
    like = lambda width, kind: jax.ShapeDtypeStruct((tokens.shape[0], width), kind)
    normed, inverse = by_rows(
        norm_kernel, "norm", [like(tokens.shape[1], jnp.bfloat16), like(1, jnp.float32)], (tokens, gain_row)
    )
    gathered = lax.all_gather(normed, Z, axis=0, tiled=True)

    place = jnp.stack([lax.axis_index(Y), lax.axis_index(X), c, x])
    halves = cotangent.reshape(2, -1, cotangent.shape[1])
    got = lax.ppermute(pick(halves, 1 - x, 0), XL, SWAP)
    plane, got = gather_plane(jnp.concatenate([w_query, key_weight, value_weight], 1), got)
    other = lax.ppermute(plane, CORE, SWAP)

    in_heads = lambda v: v.reshape(-1, SEQ, v.shape[-1])
    own, got = in_heads(pick(halves, x, 0)), in_heads(got)
    cosine, sine = rotary_tables()
    att, sent, joined, dn, gain = block(place, gathered, plane, other, own, got, cosine, sine)
    scattered = lax.psum_scatter(dn, Z, scatter_dimension=0, tiled=True)

    back = lax.ppermute(sent, XL, SWAP)

    barrier = lax.optimization_barrier
    flip = lambda v, name, size, step: lax.ppermute(v, name, [(i, i ^ step) for i in range(size)])
    wide, few = w_query.shape[1], key_weight.shape[1]
    got = [flip(gain, Z, 8, step) for step in (2, 4, 6)]
    own, other = projection_grads(place, gathered, joined, depth, wide)
    own, other, got, back = barrier((own, other, got, back))
    gain = (gain + got[0]) + (got[1] + got[2])
    got = [flip(gain, Z, 8, 1), lax.ppermute(gain, CORE, SWAP), lax.ppermute(gain, (CORE, Z), [(i, i ^ 9) for i in range(16)])]
    moved, got = barrier((lax.ppermute(other, CORE, SWAP), got))
    gain = (gain + got[0]) + (got[1] + got[2])
    one, two = ([own[h, r].astype(jnp.float32) + moved[h, r].astype(jnp.float32) for r in range(4)] for h in range(2))
    mine, extra = split_in_two(gain, wide)
    got_one, gains = with_extra(one, extra, X, gain.shape[1])
    gain = cyclic_total(mine, gains, X)
    got_two = others(narrow(two), Y)
    one, two = list(total(one[0], got_one)), list(total(two[0], got_two))
    mine, extra = split_in_two(gain, wide)
    got_one, gains = with_extra(one, extra, Y, gain.shape[1])
    got_two = others(narrow(two), X)
    (grad_tokens,) = by_rows(
        norm_back_kernel, "norm_back", [like(tokens.shape[1], jnp.bfloat16)], (scattered, tokens, inverse, gain_row)
    )
    got_one, gains, got_two, grad_tokens = barrier((got_one, gains, got_two, grad_tokens))
    grad_pre = cyclic_total(mine, gains, Y)[0] / pre_gain
    grad_query, grad_rest = total(one[0], got_one), total(two[0], got_two)
    grad_key, grad_value = grad_rest[:, :few], grad_rest[:, few:]

    attended = jnp.zeros((2,) + att.shape, att.dtype)
    attended = lax.dynamic_update_index_in_dim(attended, att, x, 0)
    attended = lax.dynamic_update_index_in_dim(attended, back, 1 - x, 0).reshape(cotangent.shape)

    return (attended, grad_tokens, grad_query, grad_key, grad_value, grad_pre)


def solution(mesh):
    torus = Mesh(mesh.devices.reshape(4, 2, 2, 2, 8), ALL)
    dp, tensor = (Y, XH, CORE), (XL, Z)
    in_specs = (P(ALL, None), P(dp, tensor), P(), P(dp, tensor), P(dp, tensor), P(dp, tensor))
    out_specs = (P(dp, tensor), P(ALL, None), P(dp, tensor), P(dp, tensor), P(dp, tensor), P())
    return jax.shard_map(per_device, mesh=torus, in_specs=in_specs, out_specs=out_specs, check_vma=False)
```
